32 devices in a mesh: wa: 8 (over z, x), ga: 4 (over y, core).
Axes of the slice: x: 2, y: 2, z: 4, core: 2. Of those that a mesh axis runs over, the one named last changes fastest.
Arguments:
- plane_ids: int32 [192], P(('ga', 'wa')), may hold values from 0 to 191, each once
- weighting: float32 [192, 256, 256], P(('ga', 'wa')), may hold values from -5 to 5
Outputs:
- kernel_table: bfloat16 [192, 64, 2048], P(None, 'wa')
The draws below stay inside these ranges and needn't reach their ends.
Inputs may be any that keep to these rules, and one draw needn't show every extreme that they name: `plane_ids`: every plane number appears in exactly one slot.
All inputs are finite; a program needn't handle non-finite values.
Results may differ from the reference program's by a relative error of at most 0.003.
Values may be sent and summed in bfloat16 or wider, within the bound.
A program may use at most 64 MiB of HBM per device.

```python
import math
import jax
import jax.numpy as jnp
from jax import lax

M = 256
OS = 8
S = 32
W = 192


def draw_weighting(key, part):
    offsets = jnp.arange(M, dtype=jnp.float32) - M // 2
    radius_scale = 2.0 * (M / 2.0) * (M / 2.0)
    radial = (offsets[:, None] ** 2 + offsets[None, :] ** 2) / radius_scale
    profile = 0.4 + 1.2 * radial * radial
    samples = jnp.clip(jax.random.normal(key, (W, M, M), jnp.float32), -3.0, 3.0)
    return samples * profile[None]


def setup_inputs(seed: int = 0) -> dict:
    keys = jax.random.split(jax.random.key(seed), 3)
    return {
        "plane_ids": jax.random.permutation(keys[0], W).astype(jnp.int32),
        "weighting": draw_weighting(jax.random.fold_in(keys[2], 71), 0),
    }


field_width = 0.2
w_top = 2000.0

def dft_tables(pixels, support, factor):
    offsets = jnp.arange(pixels, dtype=jnp.int32) - pixels // 2
    rows = jnp.arange(factor * support, dtype=jnp.int32)
    freq = (rows % support - support // 2) * factor + rows // support
    period = pixels * factor
    product = freq[:, None] * offsets[None, :] % period
    beta = 2.0 * math.pi * product.astype(jnp.float32) / period
    return (jnp.cos(beta), -jnp.sin(beta), offsets)

def plane_kernel(plane, screen, f_re, f_im, offsets, total, pixels, support, factor):
    hi = lax.Precision.HIGHEST
    coord = offsets.astype(jnp.float32) / pixels * field_width
    radius = coord[:, None] ** 2 + coord[None, :] ** 2
    nterm = jnp.sqrt(1.0 - radius) - 1.0
    wvalue = w_top * plane.astype(jnp.float32) / total
    theta = 2.0 * math.pi * wvalue * nterm
    g_re = screen * jnp.cos(theta)
    g_im = -screen * jnp.sin(theta)
    h_re = jnp.dot(g_re, f_re.T, precision=hi) - jnp.dot(g_im, f_im.T, precision=hi)
    h_im = jnp.dot(g_re, f_im.T, precision=hi) + jnp.dot(g_im, f_re.T, precision=hi)
    k_re = (jnp.dot(f_re, h_re, precision=hi) - jnp.dot(f_im, h_im, precision=hi)) / pixels
    k_im = (jnp.dot(f_re, h_im, precision=hi) + jnp.dot(f_im, h_re, precision=hi)) / pixels
    stacked = jnp.stack([k_re, k_im]).reshape(2, factor, support, factor, support)
    stacked = stacked.transpose(1, 3, 0, 2, 4).reshape(factor * factor, 2 * support * support)
    return stacked.astype(jnp.bfloat16)

def reference(plane_ids, weighting):
    f_re, f_im, offsets = dft_tables(M, S, OS)

    def one_plane(pair):
        return plane_kernel(pair[0], pair[1], f_re, f_im, offsets, W, M, S, OS)
    return lax.map(one_plane, (plane_ids, weighting))
```

```python
import functools
import math

import jax
import jax.numpy as jnp
import numpy as np
from jax import lax
from jax.experimental import pallas as pl
from jax.experimental.pallas import tpu as pltpu
from jax.sharding import PartitionSpec as P

OS = 8
S = 32
RANK = 64
LANES = 128

field_width = 0.2
w_top = 2000.0


def split(x):
    hi = x.astype(jnp.bfloat16)
    lo = (x - hi.astype(jnp.float32)).astype(jnp.bfloat16)
    return hi, lo


def np_split(x):
    hi = np.asarray(x, np.float32).astype(jnp.bfloat16)
    lo = (x - hi.astype(np.float64)).astype(np.float32).astype(jnp.bfloat16)
    return hi, lo


@functools.lru_cache(None)
def factors(pixels):
    x = np.arange(pixels) - pixels // 2
    rows = np.arange(OS * S)
    u = (rows % S - S // 2) * OS + rows // S
    period = pixels * OS
    f = np.exp(-2j * np.pi * (u[:, None] * x[None, :] % period) / period)
    half = np.exp(1j * np.pi * x / period)
    centred = f / half[None, :]
    _, _, vh = np.linalg.svd(np.concatenate([centred.real, centred.imag], 0), full_matrices=False)
    v = vh[:RANK].T
    p = centred @ v
    return v, p.real, p.imag


def tables(pixels):
    v, pr, pi = factors(pixels)
    zero = np.zeros_like(v)
    q_re = np_split(np.concatenate([v, zero], 1))
    q_im = np_split(np.concatenate([zero, v], 1))
    vt = np_split(v.T)
    order = np.arange(OS * S).reshape(OS, S // 4, 4).transpose(0, 2, 1).reshape(-1)
    left = np_split(np.concatenate([pr, pi], 1)[order] / pixels)
    right = np.concatenate(
        [np.concatenate([pr.T, pi.T], 1), np.concatenate([-pi.T, pr.T], 1)], 0
    )
    coord = (np.arange(pixels) - pixels // 2) / pixels * field_width
    radius = coord[:, None] ** 2 + coord[None, :] ** 2
    nterm = (-radius / (1.0 + np.sqrt(1.0 - radius))).astype(np.float32)
    return q_re + q_im + vt + left, np_split(right), nterm


def dot3(a, b):
    def dot(x, y):
        return jnp.dot(x, y, preferred_element_type=jnp.float32)

    return dot(a[0], b[0]) + dot(a[0], b[1]) + dot(a[1], b[0])


def half_kernel(
    total, planes, weight, nterm, qrh, qrl, qih, qil, vth, vtl, lh, ll, out, grh, grl, gih, gil
):
    pixels = weight.shape[1]
    step = 32
    wvalue = w_top * planes[pl.program_id(0)].astype(jnp.float32) / total

    @pl.loop(0, pixels // step)
    def _(chunk):
        start = pl.multiple_of(chunk * step, step)
        rows = pl.ds(start, step)
        iota = lambda d: lax.broadcasted_iota(jnp.int32, (step, pixels), d)
        shift = (iota(0) + iota(1) + (start - pixels)).astype(jnp.float32) / (2 * pixels * OS)
        turns = wvalue * nterm[rows, :]
        frac = turns - jnp.round(turns) - shift
        frac = frac - jnp.round(frac)
        y = math.pi * frac
        z = y * y
        s = jnp.full_like(z, -1.0 / math.factorial(11))
        for k in (9, 7, 5, 3, 1):
            s = s * z + (-1.0) ** (k // 2) / math.factorial(k)
        s = s * y
        c = jnp.full_like(z, 1.0 / math.factorial(12))
        for k in (10, 8, 6, 4, 2, 0):
            c = c * z + (-1.0) ** (k // 2) / math.factorial(k)
        w = weight[0, rows, :]
        g_re = w * (1.0 - 2.0 * s * s)
        g_im = w * (-2.0 * s * c)
        grh[rows, :], grl[rows, :] = split(g_re)
        gih[rows, :], gil[rows, :] = split(g_im)

    t = dot3((grh[...], grl[...]), (qrh[...], qrl[...]))
    t += dot3((gih[...], gil[...]), (qih[...], qil[...]))
    core = dot3((vth[...], vtl[...]), split(t))
    lane = lax.broadcasted_iota(jnp.int32, core.shape, 1)
    turned = pltpu.roll(core, RANK, 1)
    turned = jnp.where(lane < RANK, -turned, turned)
    stacked = jnp.concatenate([core, turned], 0)
    a = dot3((lh[...], ll[...]), split(stacked))
    out[...] = a.reshape(out.shape)


def half_transform(plane_ids, weighting, total, small, nterm):
    slots, pixels = weighting.shape[:2]
    whole = lambda a: pl.BlockSpec(a.shape, lambda s, p: (0,) * a.ndim)
    args = (nterm,) + small
    return pl.pallas_call(
        functools.partial(half_kernel, total),
        grid_spec=pltpu.PrefetchScalarGridSpec(
            num_scalar_prefetch=1,
            grid=(slots,),
            in_specs=[pl.BlockSpec((1, pixels, pixels), lambda s, p: (s, 0, 0))]
            + [whole(a) for a in args],
            out_specs=pl.BlockSpec((OS, 1, S, LANES), lambda s, p: (0, s, 0, 0)),
            scratch_shapes=[pltpu.VMEM((pixels, pixels), jnp.bfloat16)] * 4,
        ),
        out_shape=jax.ShapeDtypeStruct((OS, slots, S, LANES), jnp.float32),
        name="half_transform",
    )(plane_ids, weighting, *args)


def expand_kernel(kept, x, th, tl, out, full, mixed):
    count = x.shape[0]
    group = 2
    flat = x[...].reshape(count * S, LANES)
    full[...] = dot3(split(flat), (th[...], tl[...])).reshape(full.shape)
    lane = lax.broadcasted_iota(jnp.int32, (group * 8, LANES), 1) // S

    @pl.loop(0, count // group)
    def _(i):
        slots = pl.ds(i * group, group)
        for comp in range(2):
            for half in range(2):
                tile = comp * 2 + half
                cols = slice(tile * LANES, (tile + 1) * LANES)
                src = [
                    full[slots, c * 8 : (c + 1) * 8, cols].reshape(group * 8, LANES)
                    for c in range(4)
                ]
                src = [src[0]] + [pltpu.roll(src[c], S * c, 1) for c in range(1, 4)]
                for m in range(4):
                    kr = half * 4 + m
                    if kr >= kept:
                        continue
                    y = src[(3 - m) % 4]
                    for b in range(3):
                        y = jnp.where(lane == b, src[(b - m) % 4], y)
                    if m:
                        y = pltpu.roll(y, LANES - S * m, 1)
                    mixed[slots, comp, pl.ds(kr, 8, stride=kept), :] = y.reshape(group, 8, LANES)
        out[slots] = mixed[slots].reshape(group, 16 * kept, LANES).astype(out.dtype)


def expand(arrived, right, kept, count):
    total = arrived.shape[0]
    whole = lambda a: pl.BlockSpec(a.shape, lambda i: (0,) * a.ndim)
    return pl.pallas_call(
        functools.partial(expand_kernel, kept),
        grid=(total // count,),
        in_specs=[pl.BlockSpec((count, S, LANES), lambda i: (i, 0, 0))] + [whole(a) for a in right],
        out_specs=pl.BlockSpec((count, 16 * kept, LANES), lambda i: (i, 0, 0)),
        out_shape=jax.ShapeDtypeStruct((total, 16 * kept, LANES), jnp.bfloat16),
        scratch_shapes=[
            pltpu.VMEM((count, S, 4 * LANES), jnp.float32),
            pltpu.VMEM((count, 2, 8 * kept, LANES), jnp.float32),
        ],
        name="expand",
    )(arrived, *right)


def regroup(halves):
    moved = lax.all_to_all(halves, "wa", split_axis=0, concat_axis=0, tiled=True)
    return lax.all_gather(moved, "ga", axis=0, tiled=True)


def shards(plane_ids, weighting):
    slots, pixels = weighting.shape[:2]
    wa_count = lax.axis_size("wa")
    ga_count = lax.axis_size("ga")
    total = slots * wa_count * ga_count
    kept = OS * OS // wa_count
    small, right, nterm = tables(pixels)
    halves = half_transform(plane_ids, weighting, total, small, nterm)
    if kept < OS:
        halves = jnp.repeat(halves, OS // kept, axis=0)
        start = lax.axis_index("wa") * kept % OS
        turn = lambda t: jnp.roll(t.reshape(LANES, 2, OS, S), -start, 2).reshape(t.shape)
        right = tuple(turn(jnp.asarray(t)) for t in right)
    arrived = regroup(halves).reshape(total, S, LANES)
    table = expand(arrived, right, kept, 4 * slots)
    table = table.reshape(total, 16, kept, LANES).transpose(0, 2, 1, 3)
    return table.reshape(total, kept, 2 * S * S)


def solution(mesh):
    return jax.shard_map(
        shards,
        mesh=mesh,
        in_specs=(P(("ga", "wa")), P(("ga", "wa"), None, None)),
        out_specs=P(None, "wa", None),
        check_vma=False,
    )
```

```python
import functools
import math

import jax
import jax.numpy as jnp
import numpy as np
from jax import lax
from jax.experimental import pallas as pl
from jax.experimental.pallas import tpu as pltpu
from jax.sharding import PartitionSpec as P

OS = 8
S = 32
RANK = 64
LANES = 128
GROUPS = 3
AXES = ("wa", "ga")

field_width = 0.2
w_top = 2000.0


def split(x):
    hi = x.astype(jnp.bfloat16)
    lo = (x - hi.astype(jnp.float32)).astype(jnp.bfloat16)
    return hi, lo


def np_split(x):
    hi = np.asarray(x, np.float32).astype(jnp.bfloat16)
    lo = (x - hi.astype(np.float64)).astype(np.float32).astype(jnp.bfloat16)
    return hi, lo


@functools.lru_cache(None)
def factors(pixels):
    x = np.arange(pixels) - pixels // 2
    rows = np.arange(OS * S)
    u = (rows % S - S // 2) * OS + rows // S
    period = pixels * OS
    f = np.exp(-2j * np.pi * (u[:, None] * x[None, :] % period) / period)
    half = np.exp(1j * np.pi * x / period)
    centred = f / half[None, :]
    _, _, vh = np.linalg.svd(np.concatenate([centred.real, centred.imag], 0), full_matrices=False)
    v = vh[:RANK].T
    p = centred @ v
    return v, p.real, p.imag


def columns(real, imag):
    h = RANK // 2
    return np.concatenate([real[:, :h], imag[:, :h], real[:, h:], imag[:, h:]], 1)


def tables(pixels):
    v, pr, pi = factors(pixels)
    zero = np.zeros_like(v)
    q_re = np_split(columns(v, zero))
    q_im = np_split(columns(zero, v))
    vt = np_split(v.T)
    order = np.arange(OS * S).reshape(OS, S // 4, 4).transpose(0, 2, 1).reshape(-1)
    left = np_split(np.concatenate([pr, pi], 1)[order] / pixels)
    real, imag = np.concatenate([pr, pi]), np.concatenate([-pi, pr])
    right = columns(real, imag).T
    right_hi, right_lo = np_split(right)
    zeros = np.zeros_like(right_hi[:RANK])
    low = np.concatenate([right_hi[:RANK], zeros]), np.concatenate([zeros, right_hi[:RANK]])
    coord = (np.arange(pixels) - pixels // 2) / pixels * field_width
    radius = coord[:, None] ** 2 + coord[None, :] ** 2
    nterm = (-radius / (1.0 + np.sqrt(1.0 - radius))).astype(np.float32)
    return q_re + q_im + vt + left, (right_hi, right_lo) + low, nterm


def dot3(a, b):
    def dot(x, y):
        return jnp.dot(x, y, preferred_element_type=jnp.float32)

    return dot(a[0], b[0]) + dot(a[0], b[1]) + dot(a[1], b[0])


def half_plane(wvalue, weight, s, nterm, small, planes, sent):
    pixels = weight.shape[1]
    step = 32
    qrh, qrl, qih, qil, vth, vtl, lh, ll = small
    grh, grl, gih, gil = planes

    @pl.loop(0, pixels // step)
    def _(chunk):
        start = pl.multiple_of(chunk * step, step)
        rows = pl.ds(start, step)
        iota = lambda d: lax.broadcasted_iota(jnp.int32, (step, pixels), d)
        shift = (iota(0) + iota(1) + (start - pixels)).astype(jnp.float32) / (2 * pixels * OS)
        turns = wvalue * nterm[rows, :]
        frac = turns - jnp.round(turns) - shift
        frac = frac - jnp.round(frac)
        y = math.pi * frac
        z = y * y
        si = jnp.full_like(z, -1.0 / math.factorial(11))
        for k in (9, 7, 5, 3, 1):
            si = si * z + (-1.0) ** (k // 2) / math.factorial(k)
        si = si * y
        co = jnp.full_like(z, 1.0 / math.factorial(12))
        for k in (10, 8, 6, 4, 2, 0):
            co = co * z + (-1.0) ** (k // 2) / math.factorial(k)
        w = weight[s, rows, :]
        g_re = w * (1.0 - 2.0 * si * si)
        g_im = w * (-2.0 * si * co)
        grh[rows, :], grl[rows, :] = split(g_re)
        gih[rows, :], gil[rows, :] = split(g_im)

    t = dot3((grh[...], grl[...]), (qrh[...], qrl[...]))
    t += dot3((gih[...], gil[...]), (qih[...], qil[...]))
    core = dot3((vth[...], vtl[...]), split(t))
    lane = lax.broadcasted_iota(jnp.int32, core.shape, 1)
    quarter = RANK // 2
    turned = jnp.where(
        lane // quarter % 2 == 0,
        -pltpu.roll(core, LANES - quarter, 1),
        pltpu.roll(core, quarter, 1),
    )
    a = dot3((lh[...], ll[...]), split(jnp.concatenate([core, turned], 0)))
    hi = a.astype(jnp.bfloat16)
    lo = (a - hi.astype(jnp.float32)).reshape(OS, 2, S // 2, LANES)
    first, second = lo[:, 0].reshape(-1, LANES), lo[:, 1].reshape(-1, LANES)
    lane = lax.broadcasted_iota(jnp.int32, first.shape, 1)
    packed = jnp.where(lane < RANK, first, pltpu.roll(second, RANK, 1)).astype(jnp.bfloat16)
    sent[:, s, 0:S, :] = hi.reshape(OS, S, LANES)
    sent[:, s, S : S + S // 2, :] = packed.reshape(OS, S // 2, LANES)


def exchange_kernel(total, groups, planes_ref, weight, nterm, *refs):
    small, (held, sent, grh, grl, gih, gil), sems = refs[:8], refs[8:14], refs[14:]
    ga_count, wa_count, slots = held.shape[:3]
    per = slots // groups
    kept = OS * OS // wa_count
    w_me, g_me = lax.axis_index("wa"), lax.axis_index("ga")
    g_far = (g_me + 2) % ga_count
    g_near = g_me + 1 - 2 * (g_me % 2)
    g_cross = (g_near + 2) % ga_count

    def remote(kind, group, w_block, g_block, w_to, g_to, src=None, slot=None):
        part = pl.ds(group * per, per)
        place = held.at[g_block, w_block, part]
        return pltpu.make_async_remote_copy(
            src_ref=place if src is None else src,
            dst_ref=place,
            send_sem=sems[2 * kind].at[group, w_block if slot is None else slot],
            recv_sem=sems[2 * kind + 1].at[group, w_block],
            device_id=(w_to, g_to) if AXES[0] == "wa" else (g_to, w_to),
            device_id_type=pl.DeviceIdType.MESH,
        )

    def spread(group, w_to):
        src = sent.at[w_to * kept // OS, pl.ds(group * per, per)]
        return remote(0, group, w_me, g_me, w_to, g_me, src, w_to)

    def arrived(group, w_from):
        return remote(0, group, w_from, g_me, w_from, g_me)

    def far(group, w, g):
        return remote(1, group, w, g, w_me, g_far)

    def near(group, w, g):
        return remote(2, group, w, g, w_me, g_near)

    def near_far(group, w, g):
        return remote(3, group, w, g, w_me, g_near)

    barrier = pltpu.get_barrier_semaphore()

    def greet(w, g):
        device = (w, g) if AXES[0] == "wa" else (g, w)
        pl.semaphore_signal(barrier, inc=1, device_id=device, device_id_type=pl.DeviceIdType.MESH)

    @pl.loop(1, wa_count)
    def _(d):
        greet((w_me + d) % wa_count, g_me)

    greet(w_me, g_far)
    greet(w_me, g_near)

    def compute(group):
        @pl.loop(0, per)
        def _(i):
            s = group * per + i
            wvalue = w_top * planes_ref[s].astype(jnp.float32) / total
            half_plane(wvalue, weight, s, nterm, small, (grh, grl, gih, gil), sent)

        part = pl.ds(group * per, per)
        held[g_me, w_me, part] = sent[w_me * kept // OS, part]

    def spread_all(group):
        @pl.loop(1, wa_count)
        def _(d):
            spread(group, (w_me + d) % wa_count).start()

    def forward(group):
        near(group, w_me, g_me).start()
        far(group, w_me, g_me).start()

        @pl.loop(1, wa_count)
        def _(d):
            w = (w_me + wa_count - d) % wa_count
            arrived(group, w).wait_recv()
            far(group, w, g_me).start()
            near(group, w, g_me).start()

    def forward_far(group):
        @pl.loop(0, wa_count)
        def _(d):
            w = (w_me + wa_count - d) % wa_count
            far(group, w, g_far).wait_recv()
            near_far(group, w, g_far).start()

    compute(0)
    pl.semaphore_wait(barrier, wa_count + 1)
    spread_all(0)

    @pl.loop(1, groups)
    def _(group):
        compute(group)
        spread_all(group)
        forward(group - 1)

        @pl.when(group > 1)
        def _():
            forward_far(group - 2)

    forward(groups - 1)
    if groups > 1:
        forward_far(groups - 2)
    forward_far(groups - 1)

    @pl.loop(0, groups)
    def _(group):
        @pl.loop(1, wa_count)
        def _(d):
            spread(group, (w_me + d) % wa_count).wait_send()

        @pl.loop(0, wa_count)
        def _(w):
            far(group, w, g_me).wait_send()
            near(group, w, g_me).wait_send()
            near_far(group, w, g_far).wait_send()
            near(group, w, g_near).wait_recv()
            near_far(group, w, g_cross).wait_recv()


def exchange(plane_ids, weighting, total, small, nterm, ga_count, wa_count):
    slots, pixels = weighting.shape[:2]
    rows = S + S // 2
    groups = GROUPS if wa_count <= OS and slots % GROUPS == 0 else 1
    vmem = pl.BlockSpec(memory_space=pltpu.VMEM)
    return pl.pallas_call(
        functools.partial(exchange_kernel, total, groups),
        in_specs=[pl.BlockSpec(memory_space=pltpu.SMEM)] + [vmem] * (2 + len(small)),
        out_specs=vmem,
        out_shape=jax.ShapeDtypeStruct((ga_count, wa_count, slots, rows, LANES), jnp.bfloat16),
        scratch_shapes=[pltpu.VMEM((OS, slots, rows, LANES), jnp.bfloat16)]
        + [pltpu.VMEM((pixels, pixels), jnp.bfloat16)] * 4
        + [pltpu.SemaphoreType.DMA((groups, wa_count))] * 8,
        compiler_params=pltpu.CompilerParams(collective_id=0, has_side_effects=True),
        name="exchange",
    )(plane_ids, weighting, nterm, *small)


def expand_kernel(kept, x, th, tl, ta, tb, out, full, mixed):
    count = x.shape[0]
    group = 2
    half_rows = S // 2

    def dot(a, b):
        return jnp.dot(a, b[...], preferred_element_type=jnp.float32)

    hi = x[:, 0:S, :].reshape(count * S, LANES)
    lo = x[:, S : S + half_rows, :].reshape(count * half_rows, LANES)
    main = (dot(hi, th) + dot(hi, tl)).reshape(full.shape)
    full[:, 0:half_rows] = main[:, 0:half_rows] + dot(lo, ta).reshape(count, half_rows, -1)
    full[:, half_rows:S] = main[:, half_rows:S] + dot(lo, tb).reshape(count, half_rows, -1)
    lane = lax.broadcasted_iota(jnp.int32, (group * 8, LANES), 1) // S

    @pl.loop(0, count // group)
    def _(i):
        slots = pl.ds(i * group, group)
        for comp in range(2):
            for half in range(2):
                tile = comp * 2 + half
                cols = slice(tile * LANES, (tile + 1) * LANES)
                src = [
                    full[slots, c * 8 : (c + 1) * 8, cols].reshape(group * 8, LANES)
                    for c in range(4)
                ]
                src = [src[0]] + [pltpu.roll(src[c], S * c, 1) for c in range(1, 4)]
                for m in range(4):
                    kr = half * 4 + m
                    if kr >= kept:
                        continue
                    y = src[(3 - m) % 4]
                    for b in range(3):
                        y = jnp.where(lane == b, src[(b - m) % 4], y)
                    if m:
                        y = pltpu.roll(y, LANES - S * m, 1)
                    mixed[slots, comp, pl.ds(kr, 8, stride=kept), :] = y.reshape(group, 8, LANES)
        out[slots] = mixed[slots].reshape(group, 16 * kept, LANES).astype(out.dtype)


def expand(arrived, right, kept, count):
    total = arrived.shape[0]
    whole = lambda a: pl.BlockSpec(a.shape, lambda i: (0,) * a.ndim)
    return pl.pallas_call(
        functools.partial(expand_kernel, kept),
        grid=(total // count,),
        in_specs=[pl.BlockSpec((count,) + arrived.shape[1:], lambda i: (i, 0, 0))]
        + [whole(a) for a in right],
        out_specs=pl.BlockSpec((count, 16 * kept, LANES), lambda i: (i, 0, 0)),
        out_shape=jax.ShapeDtypeStruct((total, 16 * kept, LANES), jnp.bfloat16),
        scratch_shapes=[
            pltpu.VMEM((count, S, 4 * LANES), jnp.float32),
            pltpu.VMEM((count, 2, 8 * kept, LANES), jnp.float32),
        ],
        name="expand",
    )(arrived, *right)


def shards(plane_ids, weighting):
    slots, pixels = weighting.shape[:2]
    wa_count = lax.axis_size("wa")
    ga_count = lax.axis_size("ga")
    total = slots * wa_count * ga_count
    kept = OS * OS // wa_count
    small, right, nterm = tables(pixels)
    if kept < OS:
        start = lax.axis_index("wa") * kept % OS
        turn = lambda t: jnp.roll(t.reshape(LANES, 2, OS, S), -start, 2).reshape(t.shape)
        right = tuple(turn(jnp.asarray(t)) for t in right)
    arrived = exchange(plane_ids, weighting, total, small, nterm, ga_count, wa_count)
    arrived = arrived.reshape((total,) + arrived.shape[3:])
    table = expand(arrived, right, kept, 4 * slots)
    table = table.reshape(total, 16, kept, LANES).transpose(0, 2, 1, 3)
    return table.reshape(total, kept, 2 * S * S)


def solution(mesh):
    return jax.shard_map(
        shards,
        mesh=mesh,
        in_specs=(P(("ga", "wa")), P(("ga", "wa"), None, None)),
        out_specs=P(None, "wa", None),
        check_vma=False,
    )
```

```python
import functools
import math

import jax
import jax.numpy as jnp
import numpy as np
from jax import lax
from jax.experimental import pallas as pl
from jax.experimental.pallas import tpu as pltpu
from jax.sharding import PartitionSpec as P

OS = 8
S = 32
RANK = 64
LANES = 128
GROUPS = 3
AXES = ("wa", "ga")

field_width = 0.2
w_top = 2000.0


def split(x):
    hi = x.astype(jnp.bfloat16)
    lo = (x - hi.astype(jnp.float32)).astype(jnp.bfloat16)
    return hi, lo


def np_split(x):
    hi = np.asarray(x, np.float32).astype(jnp.bfloat16)
    lo = (x - hi.astype(np.float64)).astype(np.float32).astype(jnp.bfloat16)
    return hi, lo


@functools.lru_cache(None)
def factors(pixels):
    x = np.arange(pixels) - pixels // 2
    rows = np.arange(OS * S)
    u = (rows % S - S // 2) * OS + rows // S
    period = pixels * OS
    f = np.exp(-2j * np.pi * (u[:, None] * x[None, :] % period) / period)
    half = np.exp(1j * np.pi * x / period)
    centred = f / half[None, :]
    _, _, vh = np.linalg.svd(np.concatenate([centred.real, centred.imag], 0), full_matrices=False)
    v = vh[:RANK].T
    p = centred @ v
    return v, p.real, p.imag


def columns(real, imag):
    h = RANK // 2
    return np.concatenate([real[:, :h], imag[:, :h], real[:, h:], imag[:, h:]], 1)


def tables(pixels):
    v, pr, pi = factors(pixels)
    zero = np.zeros_like(v)
    q_re = np_split(columns(v, zero))
    q_im = np_split(columns(zero, v))
    vt = np_split(v.T)
    order = np.arange(OS * S).reshape(OS, S // 4, 4).transpose(0, 2, 1).reshape(-1)
    left = np_split(np.concatenate([pr, pi], 1)[order] / pixels)
    real, imag = np.concatenate([pr, pi]), np.concatenate([-pi, pr])
    right = columns(real, imag).T
    right_hi, right_lo = np_split(right)
    zeros = np.zeros_like(right_hi[:RANK])
    low = np.concatenate([right_hi[:RANK], zeros]), np.concatenate([zeros, right_hi[:RANK]])
    coord = (np.arange(pixels) - pixels // 2) / pixels * field_width
    radius = coord[:, None] ** 2 + coord[None, :] ** 2
    index = np.arange(pixels) - pixels // 2
    shift = (index[:, None] + index[None, :]) / (2 * pixels * OS)
    nterm = np.stack([-radius / (1.0 + np.sqrt(1.0 - radius)), shift]).astype(np.float32)
    left = left[0], np.concatenate(left, 1)
    return q_re + q_im + vt + left, (np.concatenate([right_hi, right_lo]),) + low, nterm


def dot3(a, b):
    def dot(x, y):
        return jnp.dot(x, y, preferred_element_type=jnp.float32)

    return dot(a[0], b[0]) + dot(a[0], b[1]) + dot(a[1], b[0])


def half_plane(wvalue, weight, s, nterm, small, planes, sent):
    pixels = weight.shape[1]
    step = 64
    qrh, qrl, qih, qil, vth, vtl, lh, ll = small
    grh, grl, gih, gil = planes

    @pl.loop(0, pixels // step)
    def _(chunk):
        start = pl.multiple_of(chunk * step, step)
        rows = pl.ds(start, step)
        turns = wvalue * nterm[0, rows, :] - nterm[1, rows, :]
        frac = turns - jnp.round(turns)
        y = math.pi * frac
        z = y * y
        si = jnp.full_like(z, -1.0 / math.factorial(11))
        for k in (9, 7, 5, 3, 1):
            si = si * z + (-1.0) ** (k // 2) / math.factorial(k)
        si = si * y
        co = jnp.full_like(z, 1.0 / math.factorial(12))
        for k in (10, 8, 6, 4, 2, 0):
            co = co * z + (-1.0) ** (k // 2) / math.factorial(k)
        w = weight[s, rows, :]
        g_re = w * (1.0 - 2.0 * si * si)
        g_im = w * (-2.0 * si * co)
        grh[rows, :], grl[rows, :] = split(g_re)
        gih[rows, :], gil[rows, :] = split(g_im)

    t = dot3((grh[...], grl[...]), (qrh[...], qrl[...]))
    t += dot3((gih[...], gil[...]), (qih[...], qil[...]))
    core = dot3((vth[...], vtl[...]), split(t))
    lane = lax.broadcasted_iota(jnp.int32, core.shape, 1)
    quarter = RANK // 2
    turned = jnp.where(
        lane // quarter % 2 == 0,
        -pltpu.roll(core, LANES - quarter, 1),
        pltpu.roll(core, quarter, 1),
    )
    xh, xl = split(jnp.concatenate([core, turned], 0))
    a = jnp.dot(ll[...], jnp.concatenate([xh, xh], 0), preferred_element_type=jnp.float32)
    a += jnp.dot(lh[...], xl, preferred_element_type=jnp.float32)
    hi = a.astype(jnp.bfloat16)
    lo = (a - hi.astype(jnp.float32)).reshape(OS, 2, S // 2, LANES)
    first, second = lo[:, 0].reshape(-1, LANES), lo[:, 1].reshape(-1, LANES)
    lane = lax.broadcasted_iota(jnp.int32, first.shape, 1)
    packed = jnp.where(lane < RANK, first, pltpu.roll(second, RANK, 1)).astype(jnp.bfloat16)
    sent[:, s, 0:S, :] = hi.reshape(OS, S, LANES)
    sent[:, s, S : S + S // 2, :] = packed.reshape(OS, S // 2, LANES)


def exchange_kernel(total, groups, planes_ref, weight, nterm, *refs):
    small, (held, sent, grh, grl, gih, gil), sems = refs[:8], refs[8:14], refs[14:]
    ga_count, wa_count, slots = held.shape[:3]
    per = slots // groups
    kept = OS * OS // wa_count
    w_me, g_me = lax.axis_index("wa"), lax.axis_index("ga")
    g_far = (g_me + 2) % ga_count
    g_near = g_me + 1 - 2 * (g_me % 2)
    g_cross = (g_near + 2) % ga_count

    def remote(kind, group, w_block, g_block, w_to, g_to, src=None, slot=None):
        part = pl.ds(group * per, per)
        place = held.at[g_block, w_block, part]
        return pltpu.make_async_remote_copy(
            src_ref=place if src is None else src,
            dst_ref=place,
            send_sem=sems[2 * kind].at[group, w_block if slot is None else slot],
            recv_sem=sems[2 * kind + 1].at[group, w_block],
            device_id=(w_to, g_to) if AXES[0] == "wa" else (g_to, w_to),
            device_id_type=pl.DeviceIdType.MESH,
        )

    def spread(group, w_to):
        src = sent.at[w_to * kept // OS, pl.ds(group * per, per)]
        return remote(0, group, w_me, g_me, w_to, g_me, src, w_to)

    def arrived(group, w_from):
        return remote(0, group, w_from, g_me, w_from, g_me)

    def far(group, w, g):
        return remote(1, group, w, g, w_me, g_far)

    def near(group, w, g):
        return remote(2, group, w, g, w_me, g_near)

    def near_far(group, w, g):
        return remote(3, group, w, g, w_me, g_near)

    barrier = pltpu.get_barrier_semaphore()

    def greet(w, g):
        device = (w, g) if AXES[0] == "wa" else (g, w)
        pl.semaphore_signal(barrier, inc=1, device_id=device, device_id_type=pl.DeviceIdType.MESH)

    @pl.loop(1, wa_count)
    def _(d):
        greet((w_me + d) % wa_count, g_me)

    greet(w_me, g_far)
    greet(w_me, g_near)

    def compute(group):
        @pl.loop(0, per)
        def _(i):
            s = group * per + i
            wvalue = w_top * planes_ref[s].astype(jnp.float32) / total
            half_plane(wvalue, weight, s, nterm, small, (grh, grl, gih, gil), sent)

        part = pl.ds(group * per, per)
        held[g_me, w_me, part] = sent[w_me * kept // OS, part]

    def spread_all(group):
        @pl.loop(1, wa_count)
        def _(d):
            spread(group, (w_me + d) % wa_count).start()

    def forward(group):
        near(group, w_me, g_me).start()
        far(group, w_me, g_me).start()

        @pl.loop(1, wa_count)
        def _(d):
            w = (w_me + wa_count - d) % wa_count
            arrived(group, w).wait_recv()
            far(group, w, g_me).start()
            near(group, w, g_me).start()

    def forward_far(group):
        @pl.loop(0, wa_count)
        def _(d):
            w = (w_me + wa_count - d) % wa_count
            far(group, w, g_far).wait_recv()
            near_far(group, w, g_far).start()

    compute(0)
    pl.semaphore_wait(barrier, wa_count + 1)
    spread_all(0)

    @pl.loop(1, groups)
    def _(group):
        compute(group)
        spread_all(group)
        forward(group - 1)

        @pl.when(group > 1)
        def _():
            forward_far(group - 2)

    forward(groups - 1)
    if groups > 1:
        forward_far(groups - 2)
    forward_far(groups - 1)

    @pl.loop(0, groups)
    def _(group):
        @pl.loop(1, wa_count)
        def _(d):
            spread(group, (w_me + d) % wa_count).wait_send()

        @pl.loop(0, wa_count)
        def _(w):
            far(group, w, g_me).wait_send()
            near(group, w, g_me).wait_send()
            near_far(group, w, g_far).wait_send()
            near(group, w, g_near).wait_recv()
            near_far(group, w, g_cross).wait_recv()


def exchange(plane_ids, weighting, total, small, nterm, ga_count, wa_count):
    slots, pixels = weighting.shape[:2]
    rows = S + S // 2
    groups = GROUPS if wa_count <= OS and slots % GROUPS == 0 else 1
    vmem = pl.BlockSpec(memory_space=pltpu.VMEM)
    return pl.pallas_call(
        functools.partial(exchange_kernel, total, groups),
        in_specs=[pl.BlockSpec(memory_space=pltpu.SMEM)] + [vmem] * (2 + len(small)),
        out_specs=vmem,
        out_shape=jax.ShapeDtypeStruct((ga_count, wa_count, slots, rows, LANES), jnp.bfloat16),
        scratch_shapes=[pltpu.VMEM((OS, slots, rows, LANES), jnp.bfloat16)]
        + [pltpu.VMEM((pixels, pixels), jnp.bfloat16)] * 4
        + [pltpu.SemaphoreType.DMA((groups, wa_count))] * 8,
        compiler_params=pltpu.CompilerParams(collective_id=0, has_side_effects=True),
        name="exchange",
    )(plane_ids, weighting, nterm, *small)


def expand_kernel(kept, x, th, ta, tb, out, full, mixed):
    count = x.shape[0]
    group = count // 4
    half_rows = S // 2

    def dot(a, b):
        return jnp.dot(a, b[...], preferred_element_type=jnp.float32)

    hi = x[:, 0:S, :].reshape(count * S, LANES)
    lo = x[:, S : S + half_rows, :].reshape(count * half_rows, LANES)
    main = dot(jnp.concatenate([hi, hi], 1), th).reshape(full.shape)
    full[:, 0:half_rows] = main[:, 0:half_rows] + dot(lo, ta).reshape(count, half_rows, -1)
    full[:, half_rows:S] = main[:, half_rows:S] + dot(lo, tb).reshape(count, half_rows, -1)
    lane = lax.broadcasted_iota(jnp.int32, (group * 8, LANES), 1) // S

    @pl.loop(0, count // group)
    def _(i):
        slots = pl.ds(i * group, group)
        for comp in range(2):
            for half in range(2):
                tile = comp * 2 + half
                cols = slice(tile * LANES, (tile + 1) * LANES)
                src = [
                    full[slots, c * 8 : (c + 1) * 8, cols].reshape(group * 8, LANES)
                    for c in range(4)
                ]
                src = [src[0]] + [pltpu.roll(src[c], S * c, 1) for c in range(1, 4)]
                for m in range(4):
                    kr = half * 4 + m
                    if kr >= kept:
                        continue
                    y = src[(3 - m) % 4]
                    for b in range(3):
                        y = jnp.where(lane == b, src[(b - m) % 4], y)
                    if m:
                        y = pltpu.roll(y, LANES - S * m, 1)
                    mixed[slots, comp, pl.ds(kr, 8, stride=kept), :] = y.reshape(group, 8, LANES)

    @pl.loop(0, count // group)
    def _(i):
        slots = pl.ds(i * group, group)
        out[slots] = mixed[slots].reshape(group, 16 * kept, LANES).astype(out.dtype)


def expand(arrived, right, kept, count):
    total = arrived.shape[0]
    whole = lambda a: pl.BlockSpec(a.shape, lambda i: (0,) * a.ndim)
    return pl.pallas_call(
        functools.partial(expand_kernel, kept),
        grid=(total // count,),
        in_specs=[pl.BlockSpec((count,) + arrived.shape[1:], lambda i: (i, 0, 0))]
        + [whole(a) for a in right],
        out_specs=pl.BlockSpec((count, 16 * kept, LANES), lambda i: (i, 0, 0)),
        out_shape=jax.ShapeDtypeStruct((total, 16 * kept, LANES), jnp.bfloat16),
        scratch_shapes=[
            pltpu.VMEM((count, S, 4 * LANES), jnp.float32),
            pltpu.VMEM((count, 2, 8 * kept, LANES), jnp.float32),
        ],
        name="expand",
    )(arrived, *right)


def shards(plane_ids, weighting):
    slots, pixels = weighting.shape[:2]
    wa_count = lax.axis_size("wa")
    ga_count = lax.axis_size("ga")
    total = slots * wa_count * ga_count
    kept = OS * OS // wa_count
    small, right, nterm = tables(pixels)
    if kept < OS:
        start = lax.axis_index("wa") * kept % OS
        turn = lambda t: jnp.roll(t.reshape(-1, 2, OS, S), -start, 2).reshape(t.shape)
        right = tuple(turn(jnp.asarray(t)) for t in right)
    arrived = exchange(plane_ids, weighting, total, small, nterm, ga_count, wa_count)
    arrived = arrived.reshape((total,) + arrived.shape[3:])
    table = expand(arrived, right, kept, 4 * slots)
    table = table.reshape(total, 16, kept, LANES).transpose(0, 2, 1, 3)
    return table.reshape(total, kept, 2 * S * S)


def solution(mesh):
    return jax.shard_map(
        shards,
        mesh=mesh,
        in_specs=(P(("ga", "wa")), P(("ga", "wa"), None, None)),
        out_specs=P(None, "wa", None),
        check_vma=False,
    )
```

```python
import functools
import math

import jax
import jax.numpy as jnp
import numpy as np
from jax import lax
from jax.experimental import pallas as pl
from jax.experimental.pallas import tpu as pltpu
from jax.sharding import PartitionSpec as P

OS = 8
S = 32
RANK = 64
LANES = 128
GROUPS = 6
AXES = ("wa", "ga")

field_width = 0.2
w_top = 2000.0


def split(x):
    hi = x.astype(jnp.bfloat16)
    lo = (x - hi.astype(jnp.float32)).astype(jnp.bfloat16)
    return hi, lo


def np_split(x):
    hi = np.asarray(x, np.float32).astype(jnp.bfloat16)
    lo = (x - hi.astype(np.float64)).astype(np.float32).astype(jnp.bfloat16)
    return hi, lo


@functools.lru_cache(None)
def factors(pixels):
    x = np.arange(pixels) - pixels // 2
    rows = np.arange(OS * S)
    u = (rows % S - S // 2) * OS + rows // S
    period = pixels * OS
    f = np.exp(-2j * np.pi * (u[:, None] * x[None, :] % period) / period)
    half = np.exp(1j * np.pi * x / period)
    centred = f / half[None, :]
    _, _, vh = np.linalg.svd(np.concatenate([centred.real, centred.imag], 0), full_matrices=False)
    v = vh[:RANK].T
    p = centred @ v
    return v, p.real, p.imag


def columns(real, imag):
    h = RANK // 2
    return np.concatenate([real[:, :h], imag[:, :h], real[:, h:], imag[:, h:]], 1)


def tables(pixels):
    v, pr, pi = factors(pixels)
    zero = np.zeros_like(v)
    q_re = np_split(columns(v, zero))
    q_im = np_split(columns(zero, v))
    vt = np_split(v.T)
    order = np.arange(OS * S).reshape(OS, S // 4, 4).transpose(0, 2, 1).reshape(-1)
    left = np_split(np.concatenate([pr, pi], 1)[order] / pixels)
    real, imag = np.concatenate([pr, pi]), np.concatenate([-pi, pr])
    right = columns(real, imag).T
    right_hi, right_lo = np_split(right)
    zeros = np.zeros_like(right_hi[:RANK])
    low = np.concatenate([right_hi[:RANK], zeros]), np.concatenate([zeros, right_hi[:RANK]])
    coord = (np.arange(pixels) - pixels // 2) / pixels * field_width
    radius = coord[:, None] ** 2 + coord[None, :] ** 2
    index = np.arange(pixels) - pixels // 2
    shift = (index[:, None] + index[None, :]) / (2 * pixels * OS)
    nterm = np.stack([-radius / (1.0 + np.sqrt(1.0 - radius)), shift]).astype(np.float32)
    left = left[0], np.concatenate(left, 1)
    return q_re + q_im + vt + left, (np.concatenate([right_hi, right_lo]),) + low, nterm


def dot3(a, b):
    def dot(x, y):
        return jnp.dot(x, y, preferred_element_type=jnp.float32)

    return dot(a[0], b[0]) + dot(a[0], b[1]) + dot(a[1], b[0])


def half_plane(wvalue, weight, s, nterm, small, planes, sent):
    pixels = weight.shape[1]
    step = 64
    qrh, qrl, qih, qil, vth, vtl, lh, ll = small
    grh, grl, gih, gil = planes

    @pl.loop(0, pixels // step)
    def _(chunk):
        start = pl.multiple_of(chunk * step, step)
        rows = pl.ds(start, step)
        turns = wvalue * nterm[0, rows, :] - nterm[1, rows, :]
        frac = turns - jnp.round(turns)
        y = math.pi * frac
        z = y * y
        si = jnp.full_like(z, -1.0 / math.factorial(11))
        for k in (9, 7, 5, 3, 1):
            si = si * z + (-1.0) ** (k // 2) / math.factorial(k)
        si = si * y
        co = jnp.full_like(z, 1.0 / math.factorial(12))
        for k in (10, 8, 6, 4, 2, 0):
            co = co * z + (-1.0) ** (k // 2) / math.factorial(k)
        w = weight[s, rows, :]
        g_re = w * (1.0 - 2.0 * si * si)
        g_im = w * (-2.0 * si * co)
        grh[rows, :], grl[rows, :] = split(g_re)
        gih[rows, :], gil[rows, :] = split(g_im)

    t = dot3((grh[...], grl[...]), (qrh[...], qrl[...]))
    t += dot3((gih[...], gil[...]), (qih[...], qil[...]))
    core = dot3((vth[...], vtl[...]), split(t))
    lane = lax.broadcasted_iota(jnp.int32, core.shape, 1)
    quarter = RANK // 2
    turned = jnp.where(
        lane // quarter % 2 == 0,
        -pltpu.roll(core, LANES - quarter, 1),
        pltpu.roll(core, quarter, 1),
    )
    xh, xl = split(jnp.concatenate([core, turned], 0))
    a = jnp.dot(ll[...], jnp.concatenate([xh, xh], 0), preferred_element_type=jnp.float32)
    a += jnp.dot(lh[...], xl, preferred_element_type=jnp.float32)
    hi = a.astype(jnp.bfloat16)
    lo = (a - hi.astype(jnp.float32)).reshape(OS, 2, S // 2, LANES)
    first, second = lo[:, 0].reshape(-1, LANES), lo[:, 1].reshape(-1, LANES)
    lane = lax.broadcasted_iota(jnp.int32, first.shape, 1)
    packed = jnp.where(lane < RANK, first, pltpu.roll(second, RANK, 1)).astype(jnp.bfloat16)
    sent[:, s, 0:S, :] = hi.reshape(OS, S, LANES)
    sent[:, s, S : S + S // 2, :] = packed.reshape(OS, S // 2, LANES)


def exchange_kernel(total, groups, planes_ref, weight, nterm, *refs):
    small, (held, sent, grh, grl, gih, gil), sems = refs[:8], refs[8:14], refs[14:]
    ga_count, wa_count, slots = held.shape[:3]
    per = slots // groups
    kept = OS * OS // wa_count
    w_me, g_me = lax.axis_index("wa"), lax.axis_index("ga")
    g_far = (g_me + 2) % ga_count
    g_near = g_me + 1 - 2 * (g_me % 2)
    g_cross = (g_near + 2) % ga_count

    def remote(kind, group, w_block, g_block, w_to, g_to, src=None, slot=None):
        part = pl.ds(group * per, per)
        place = held.at[g_block, w_block, part]
        return pltpu.make_async_remote_copy(
            src_ref=place if src is None else src,
            dst_ref=place,
            send_sem=sems[2 * kind].at[group, w_block if slot is None else slot],
            recv_sem=sems[2 * kind + 1].at[group, w_block],
            device_id=(w_to, g_to) if AXES[0] == "wa" else (g_to, w_to),
            device_id_type=pl.DeviceIdType.MESH,
        )

    def spread(group, w_to):
        src = sent.at[w_to * kept // OS, pl.ds(group * per, per)]
        return remote(0, group, w_me, g_me, w_to, g_me, src, w_to)

    def arrived(group, w_from):
        return remote(0, group, w_from, g_me, w_from, g_me)

    def far(group, w, g):
        return remote(1, group, w, g, w_me, g_far)

    def near(group, w, g):
        return remote(2, group, w, g, w_me, g_near)

    def near_far(group, w, g):
        return remote(3, group, w, g, w_me, g_near)

    barrier = pltpu.get_barrier_semaphore()

    def greet(w, g):
        device = (w, g) if AXES[0] == "wa" else (g, w)
        pl.semaphore_signal(barrier, inc=1, device_id=device, device_id_type=pl.DeviceIdType.MESH)

    @pl.loop(1, wa_count)
    def _(d):
        greet((w_me + d) % wa_count, g_me)

    greet(w_me, g_far)
    greet(w_me, g_near)

    def compute(group):
        @pl.loop(0, per)
        def _(i):
            s = group * per + i
            wvalue = w_top * planes_ref[s].astype(jnp.float32) / total
            half_plane(wvalue, weight, s, nterm, small, (grh, grl, gih, gil), sent)

        part = pl.ds(group * per, per)
        held[g_me, w_me, part] = sent[w_me * kept // OS, part]

    def spread_all(group):
        @pl.loop(1, wa_count)
        def _(d):
            spread(group, (w_me + d) % wa_count).start()

    def forward(group):
        near(group, w_me, g_me).start()
        far(group, w_me, g_me).start()

        @pl.loop(1, wa_count)
        def _(d):
            w = (w_me + wa_count - d) % wa_count
            arrived(group, w).wait_recv()
            far(group, w, g_me).start()
            near(group, w, g_me).start()

    def forward_far(group):
        @pl.loop(0, wa_count)
        def _(d):
            w = (w_me + wa_count - d) % wa_count
            far(group, w, g_far).wait_recv()
            near_far(group, w, g_far).start()

    compute(0)
    pl.semaphore_wait(barrier, wa_count + 1)
    spread_all(0)

    @pl.loop(1, groups)
    def _(group):
        compute(group)
        spread_all(group)
        forward(group - 1)

        @pl.when(group > 1)
        def _():
            forward_far(group - 2)

    forward(groups - 1)
    if groups > 1:
        forward_far(groups - 2)
    forward_far(groups - 1)

    @pl.loop(0, groups)
    def _(group):
        @pl.loop(1, wa_count)
        def _(d):
            spread(group, (w_me + d) % wa_count).wait_send()

        @pl.loop(0, wa_count)
        def _(w):
            far(group, w, g_me).wait_send()
            near(group, w, g_me).wait_send()
            near_far(group, w, g_far).wait_send()
            near(group, w, g_near).wait_recv()
            near_far(group, w, g_cross).wait_recv()


def exchange(plane_ids, weighting, total, small, nterm, ga_count, wa_count):
    slots, pixels = weighting.shape[:2]
    rows = S + S // 2
    groups = GROUPS if wa_count <= OS and slots % GROUPS == 0 else 1
    vmem = pl.BlockSpec(memory_space=pltpu.VMEM)
    return pl.pallas_call(
        functools.partial(exchange_kernel, total, groups),
        in_specs=[pl.BlockSpec(memory_space=pltpu.SMEM)] + [vmem] * (2 + len(small)),
        out_specs=vmem,
        out_shape=jax.ShapeDtypeStruct((ga_count, wa_count, slots, rows, LANES), jnp.bfloat16),
        scratch_shapes=[pltpu.VMEM((OS, slots, rows, LANES), jnp.bfloat16)]
        + [pltpu.VMEM((pixels, pixels), jnp.bfloat16)] * 4
        + [pltpu.SemaphoreType.DMA((groups, wa_count))] * 8,
        compiler_params=pltpu.CompilerParams(collective_id=0, has_side_effects=True),
        name="exchange",
    )(plane_ids, weighting, nterm, *small)


def expand_kernel(kept, x, th, ta, tb, out, full, mixed):
    count = x.shape[0]
    group = count // 4
    half_rows = S // 2

    def dot(a, b):
        return jnp.dot(a, b[...], preferred_element_type=jnp.float32)

    hi = x[:, 0:S, :].reshape(count * S, LANES)
    lo = x[:, S : S + half_rows, :].reshape(count * half_rows, LANES)
    main = dot(jnp.concatenate([hi, hi], 1), th).reshape(full.shape)
    full[:, 0:half_rows] = main[:, 0:half_rows] + dot(lo, ta).reshape(count, half_rows, -1)
    full[:, half_rows:S] = main[:, half_rows:S] + dot(lo, tb).reshape(count, half_rows, -1)
    lane = lax.broadcasted_iota(jnp.int32, (group * 8, LANES), 1) // S

    @pl.loop(0, count // group)
    def _(i):
        slots = pl.ds(i * group, group)
        for comp in range(2):
            rows = []
            for half in range(2):
                tile = comp * 2 + half
                cols = slice(tile * LANES, (tile + 1) * LANES)
                src = [
                    full[slots, c * 8 : (c + 1) * 8, cols].reshape(group * 8, LANES)
                    for c in range(4)
                ]
                src = [src[0]] + [pltpu.roll(src[c], S * c, 1) for c in range(1, 4)]
                for m in range(4):
                    kr = half * 4 + m
                    if kr >= kept:
                        continue
                    y = src[(3 - m) % 4]
                    for b in range(3):
                        y = jnp.where(lane == b, src[(b - m) % 4], y)
                    if m:
                        y = pltpu.roll(y, LANES - S * m, 1)
                    if kept == OS:
                        rows.append(y.reshape(group, 8, LANES))
                    else:
                        mixed[slots, comp, pl.ds(kr, 8, stride=kept), :] = y.reshape(group, 8, LANES)
            for k in range(group if kept == OS else 0):
                tile = jnp.swapaxes(jnp.stack([row[k] for row in rows]), 0, 1)
                part = pl.ds(comp * 8 * kept, 8 * kept)
                out[i * group + k, part] = tile.reshape(8 * kept, LANES).astype(out.dtype)

    if kept == OS:
        return

    @pl.loop(0, count // group)
    def _(i):
        slots = pl.ds(i * group, group)
        out[slots] = mixed[slots].reshape(group, 16 * kept, LANES).astype(out.dtype)


def expand(arrived, right, kept, count):
    total = arrived.shape[0]
    whole = lambda a: pl.BlockSpec(a.shape, lambda i: (0,) * a.ndim)
    return pl.pallas_call(
        functools.partial(expand_kernel, kept),
        grid=(total // count,),
        in_specs=[pl.BlockSpec((count,) + arrived.shape[1:], lambda i: (i, 0, 0))]
        + [whole(a) for a in right],
        out_specs=pl.BlockSpec((count, 16 * kept, LANES), lambda i: (i, 0, 0)),
        out_shape=jax.ShapeDtypeStruct((total, 16 * kept, LANES), jnp.bfloat16),
        scratch_shapes=[
            pltpu.VMEM((count, S, 4 * LANES), jnp.float32),
            pltpu.VMEM((count, 2, 8 * kept, LANES), jnp.float32),
        ],
        name="expand",
    )(arrived, *right)


def shards(plane_ids, weighting):
    slots, pixels = weighting.shape[:2]
    wa_count = lax.axis_size("wa")
    ga_count = lax.axis_size("ga")
    total = slots * wa_count * ga_count
    kept = OS * OS // wa_count
    small, right, nterm = tables(pixels)
    if kept < OS:
        start = lax.axis_index("wa") * kept % OS
        turn = lambda t: jnp.roll(t.reshape(-1, 2, OS, S), -start, 2).reshape(t.shape)
        right = tuple(turn(jnp.asarray(t)) for t in right)
    arrived = exchange(plane_ids, weighting, total, small, nterm, ga_count, wa_count)
    arrived = arrived.reshape((total,) + arrived.shape[3:])
    table = expand(arrived, right, kept, 4 * slots)
    table = table.reshape(total, 16, kept, LANES).transpose(0, 2, 1, 3)
    return table.reshape(total, kept, 2 * S * S)


def solution(mesh):
    return jax.shard_map(
        shards,
        mesh=mesh,
        in_specs=(P(("ga", "wa")), P(("ga", "wa"), None, None)),
        out_specs=P(None, "wa", None),
        check_vma=False,
    )
```

```python
import functools
import math

import jax
import jax.numpy as jnp
import numpy as np
from jax import lax
from jax.experimental import pallas as pl
from jax.experimental.pallas import tpu as pltpu
from jax.sharding import PartitionSpec as P

OS = 8
S = 32
RANK = 64
LANES = 128
GROUPS = 2
AXES = ("wa", "ga")

field_width = 0.2
w_top = 2000.0


def split(x):
    hi = x.astype(jnp.bfloat16)
    lo = (x - hi.astype(jnp.float32)).astype(jnp.bfloat16)
    return hi, lo


def np_split(x):
    hi = np.asarray(x, np.float32).astype(jnp.bfloat16)
    lo = (x - hi.astype(np.float64)).astype(np.float32).astype(jnp.bfloat16)
    return hi, lo


@functools.lru_cache(None)
def factors(pixels):
    x = np.arange(pixels) - pixels // 2
    rows = np.arange(OS * S)
    u = (rows % S - S // 2) * OS + rows // S
    period = pixels * OS
    f = np.exp(-2j * np.pi * (u[:, None] * x[None, :] % period) / period)
    half = np.exp(1j * np.pi * x / period)
    centred = f / half[None, :]
    _, _, vh = np.linalg.svd(np.concatenate([centred.real, centred.imag], 0), full_matrices=False)
    v = vh[:RANK].T
    p = centred @ v
    return v, p.real, p.imag


def columns(real, imag):
    h = RANK // 2
    return np.concatenate([real[:, :h], imag[:, :h], real[:, h:], imag[:, h:]], 1)


def tables(pixels):
    v, pr, pi = factors(pixels)
    zero = np.zeros_like(v)
    q_re = np_split(columns(v, zero))
    q_im = np_split(columns(zero, v))
    vt = np_split(v.T)
    order = np.arange(OS * S).reshape(OS, S // 4, 4).transpose(0, 2, 1).reshape(-1)
    left = np_split(np.concatenate([pr, pi], 1)[order] / pixels)
    real, imag = np.concatenate([pr, pi]), np.concatenate([-pi, pr])
    right = columns(real, imag).T
    right_hi, right_lo = np_split(right)
    zeros = np.zeros_like(right_hi[:RANK])
    low = np.concatenate([right_hi[:RANK], zeros]), np.concatenate([zeros, right_hi[:RANK]])
    coord = (np.arange(pixels) - pixels // 2) / pixels * field_width
    radius = coord[:, None] ** 2 + coord[None, :] ** 2
    index = np.arange(pixels) - pixels // 2
    shift = (index[:, None] + index[None, :]) / (2 * pixels * OS)
    nterm = np.stack([-radius / (1.0 + np.sqrt(1.0 - radius)), shift]).astype(np.float32)
    left = left[0], np.concatenate(left, 1)
    return q_re + q_im + vt + left, (np.concatenate([right_hi, right_lo]),) + low, nterm


def dot3(a, b):
    def dot(x, y):
        return jnp.dot(x, y, preferred_element_type=jnp.float32)

    return dot(a[0], b[0]) + dot(a[0], b[1]) + dot(a[1], b[0])


def half_plane(wvalue, weight, s, nterm, small, planes, sent):
    pixels = weight.shape[1]
    step = 64
    qrh, qrl, qih, qil, vth, vtl, lh, ll = small
    grh, grl, gih, gil = planes

    @pl.loop(0, pixels // step)
    def _(chunk):
        start = pl.multiple_of(chunk * step, step)
        rows = pl.ds(start, step)
        turns = wvalue * nterm[0, rows, :] - nterm[1, rows, :]
        frac = turns - jnp.round(turns)
        y = math.pi * frac
        z = y * y
        si = jnp.full_like(z, -1.0 / math.factorial(11))
        for k in (9, 7, 5, 3, 1):
            si = si * z + (-1.0) ** (k // 2) / math.factorial(k)
        si = si * y
        co = jnp.full_like(z, 1.0 / math.factorial(12))
        for k in (10, 8, 6, 4, 2, 0):
            co = co * z + (-1.0) ** (k // 2) / math.factorial(k)
        w = weight[s, rows, :]
        g_re = w * (1.0 - 2.0 * si * si)
        g_im = w * (-2.0 * si * co)
        grh[rows, :], grl[rows, :] = split(g_re)
        gih[rows, :], gil[rows, :] = split(g_im)

    t = dot3((grh[...], grl[...]), (qrh[...], qrl[...]))
    t += dot3((gih[...], gil[...]), (qih[...], qil[...]))
    core = dot3((vth[...], vtl[...]), split(t))
    lane = lax.broadcasted_iota(jnp.int32, core.shape, 1)
    quarter = RANK // 2
    turned = jnp.where(
        lane // quarter % 2 == 0,
        -pltpu.roll(core, LANES - quarter, 1),
        pltpu.roll(core, quarter, 1),
    )
    xh, xl = split(jnp.concatenate([core, turned], 0))
    a = jnp.dot(ll[...], jnp.concatenate([xh, xh], 0), preferred_element_type=jnp.float32)
    a += jnp.dot(lh[...], xl, preferred_element_type=jnp.float32)
    hi = a.astype(jnp.bfloat16)
    lo = (a - hi.astype(jnp.float32)).reshape(OS, 2, S // 2, LANES)
    first, second = lo[:, 0].reshape(-1, LANES), lo[:, 1].reshape(-1, LANES)
    lane = lax.broadcasted_iota(jnp.int32, first.shape, 1)
    packed = jnp.where(lane < RANK, first, pltpu.roll(second, RANK, 1)).astype(jnp.bfloat16)
    sent[:, s, 0:S, :] = hi.reshape(OS, S, LANES)
    sent[:, s, S : S + S // 2, :] = packed.reshape(OS, S // 2, LANES)


def exchange_kernel(total, groups, planes_ref, weight, nterm, *refs):
    small, (held, sent, grh, grl, gih, gil), sems = refs[:8], refs[8:14], refs[14:]
    ga_count, wa_count, slots = held.shape[:3]
    per = slots // groups
    kept = OS * OS // wa_count
    w_me, g_me = lax.axis_index("wa"), lax.axis_index("ga")
    g_far = (g_me + 2) % ga_count
    g_near = g_me + 1 - 2 * (g_me % 2)
    g_cross = (g_near + 2) % ga_count

    def remote(kind, group, w_block, g_block, w_to, g_to, src=None, slot=None):
        part = pl.ds(group * per, per)
        place = held.at[g_block, w_block, part]
        return pltpu.make_async_remote_copy(
            src_ref=place if src is None else src,
            dst_ref=place,
            send_sem=sems[2 * kind].at[group, w_block if slot is None else slot],
            recv_sem=sems[2 * kind + 1].at[group, w_block],
            device_id=(w_to, g_to) if AXES[0] == "wa" else (g_to, w_to),
            device_id_type=pl.DeviceIdType.MESH,
        )

    def spread(group, w_to):
        src = sent.at[w_to * kept // OS, pl.ds(group * per, per)]
        return remote(0, group, w_me, g_me, w_to, g_me, src, w_to)

    def arrived(group, w_from):
        return remote(0, group, w_from, g_me, w_from, g_me)

    def far(group, w, g):
        return remote(1, group, w, g, w_me, g_far)

    def near(group, w, g):
        return remote(2, group, w, g, w_me, g_near)

    def near_far(group, w, g):
        return remote(3, group, w, g, w_me, g_near)

    barrier = pltpu.get_barrier_semaphore()

    def greet(w, g):
        device = (w, g) if AXES[0] == "wa" else (g, w)
        pl.semaphore_signal(barrier, inc=1, device_id=device, device_id_type=pl.DeviceIdType.MESH)

    @pl.loop(1, wa_count)
    def _(d):
        greet((w_me + d) % wa_count, g_me)

    greet(w_me, g_far)
    greet(w_me, g_near)

    def compute(group):
        @pl.loop(0, per)
        def _(i):
            s = group * per + i
            wvalue = w_top * planes_ref[s].astype(jnp.float32) / total
            half_plane(wvalue, weight, s, nterm, small, (grh, grl, gih, gil), sent)

        part = pl.ds(group * per, per)
        held[g_me, w_me, part] = sent[w_me * kept // OS, part]

    def spread_all(group):
        @pl.loop(1, wa_count)
        def _(d):
            spread(group, (w_me + d) % wa_count).start()

    def forward(group):
        near(group, w_me, g_me).start()
        far(group, w_me, g_me).start()

        @pl.loop(1, wa_count)
        def _(d):
            w = (w_me + wa_count - d) % wa_count
            arrived(group, w).wait_recv()
            far(group, w, g_me).start()
            near(group, w, g_me).start()

    def forward_far(group):
        @pl.loop(0, wa_count)
        def _(d):
            w = (w_me + wa_count - d) % wa_count
            far(group, w, g_far).wait_recv()
            near_far(group, w, g_far).start()

    compute(0)
    pl.semaphore_wait(barrier, wa_count + 1)
    spread_all(0)

    @pl.loop(1, groups)
    def _(group):
        compute(group)
        spread_all(group)
        forward(group - 1)

        @pl.when(group > 1)
        def _():
            forward_far(group - 2)

    forward(groups - 1)
    if groups > 1:
        forward_far(groups - 2)
    forward_far(groups - 1)

    @pl.loop(0, groups)
    def _(group):
        @pl.loop(1, wa_count)
        def _(d):
            spread(group, (w_me + d) % wa_count).wait_send()

        @pl.loop(0, wa_count)
        def _(w):
            far(group, w, g_me).wait_send()
            near(group, w, g_me).wait_send()
            near_far(group, w, g_far).wait_send()
            near(group, w, g_near).wait_recv()
            near_far(group, w, g_cross).wait_recv()


def exchange(plane_ids, weighting, total, small, nterm, ga_count, wa_count):
    slots, pixels = weighting.shape[:2]
    rows = S + S // 2
    groups = GROUPS if wa_count <= OS and slots % GROUPS == 0 else 1
    vmem = pl.BlockSpec(memory_space=pltpu.VMEM)
    return pl.pallas_call(
        functools.partial(exchange_kernel, total, groups),
        in_specs=[pl.BlockSpec(memory_space=pltpu.SMEM)] + [vmem] * (2 + len(small)),
        out_specs=vmem,
        out_shape=jax.ShapeDtypeStruct((ga_count, wa_count, slots, rows, LANES), jnp.bfloat16),
        scratch_shapes=[pltpu.VMEM((OS, slots, rows, LANES), jnp.bfloat16)]
        + [pltpu.VMEM((pixels, pixels), jnp.bfloat16)] * 4
        + [pltpu.SemaphoreType.DMA((groups, wa_count))] * 8,
        compiler_params=pltpu.CompilerParams(collective_id=0, has_side_effects=True),
        name="exchange",
    )(plane_ids, weighting, nterm, *small)


def expand_kernel(kept, x, th, ta, tb, out, full, mixed):
    count = x.shape[0]
    group = count // 4
    half_rows = S // 2

    def dot(a, b):
        return jnp.dot(a, b[...], preferred_element_type=jnp.float32)

    hi = x[:, 0:S, :].reshape(count * S, LANES)
    lo = x[:, S : S + half_rows, :].reshape(count * half_rows, LANES)
    main = dot(jnp.concatenate([hi, hi], 1), th).reshape(full.shape)
    full[:, 0:half_rows] = main[:, 0:half_rows] + dot(lo, ta).reshape(count, half_rows, -1)
    full[:, half_rows:S] = main[:, half_rows:S] + dot(lo, tb).reshape(count, half_rows, -1)
    lane = lax.broadcasted_iota(jnp.int32, (group * 8, LANES), 1) // S

    @pl.loop(0, count // group)
    def _(i):
        slots = pl.ds(i * group, group)
        for comp in range(2):
            rows = []
            for half in range(2):
                tile = comp * 2 + half
                cols = slice(tile * LANES, (tile + 1) * LANES)
                src = [
                    full[slots, c * 8 : (c + 1) * 8, cols].reshape(group * 8, LANES)
                    for c in range(4)
                ]
                src = [src[0]] + [pltpu.roll(src[c], S * c, 1) for c in range(1, 4)]
                for m in range(4):
                    kr = half * 4 + m
                    if kr >= kept:
                        continue
                    y = src[(3 - m) % 4]
                    for b in range(3):
                        y = jnp.where(lane == b, src[(b - m) % 4], y)
                    if m:
                        y = pltpu.roll(y, LANES - S * m, 1)
                    if kept == OS:
                        rows.append(y.reshape(group, 8, LANES))
                    else:
                        mixed[slots, comp, pl.ds(kr, 8, stride=kept), :] = y.reshape(group, 8, LANES)
            for k in range(group if kept == OS else 0):
                tile = jnp.swapaxes(jnp.stack([row[k] for row in rows]), 0, 1)
                part = pl.ds(comp * 8 * kept, 8 * kept)
                out[i * group + k, part] = tile.reshape(8 * kept, LANES).astype(out.dtype)

    if kept == OS:
        return

    @pl.loop(0, count // group)
    def _(i):
        slots = pl.ds(i * group, group)
        out[slots] = mixed[slots].reshape(group, 16 * kept, LANES).astype(out.dtype)


def expand(arrived, right, kept, count):
    total = arrived.shape[0]
    whole = lambda a: pl.BlockSpec(a.shape, lambda i: (0,) * a.ndim)
    return pl.pallas_call(
        functools.partial(expand_kernel, kept),
        grid=(total // count,),
        in_specs=[pl.BlockSpec((count,) + arrived.shape[1:], lambda i: (i, 0, 0))]
        + [whole(a) for a in right],
        out_specs=pl.BlockSpec((count, 16 * kept, LANES), lambda i: (i, 0, 0)),
        out_shape=jax.ShapeDtypeStruct((total, 16 * kept, LANES), jnp.bfloat16),
        scratch_shapes=[
            pltpu.VMEM((count, S, 4 * LANES), jnp.float32),
            pltpu.VMEM((count, 2, 8 * kept, LANES), jnp.float32),
        ],
        name="expand",
    )(arrived, *right)


def shards(plane_ids, weighting):
    slots, pixels = weighting.shape[:2]
    wa_count = lax.axis_size("wa")
    ga_count = lax.axis_size("ga")
    total = slots * wa_count * ga_count
    kept = OS * OS // wa_count
    small, right, nterm = tables(pixels)
    if kept < OS:
        start = lax.axis_index("wa") * kept % OS
        turn = lambda t: jnp.roll(t.reshape(-1, 2, OS, S), -start, 2).reshape(t.shape)
        right = tuple(turn(jnp.asarray(t)) for t in right)
    arrived = exchange(plane_ids, weighting, total, small, nterm, ga_count, wa_count)
    arrived = arrived.reshape((total,) + arrived.shape[3:])
    table = expand(arrived, right, kept, 4 * slots)
    table = table.reshape(total, 16, kept, LANES).transpose(0, 2, 1, 3)
    return table.reshape(total, kept, 2 * S * S)


def solution(mesh):
    return jax.shard_map(
        shards,
        mesh=mesh,
        in_specs=(P(("ga", "wa")), P(("ga", "wa"), None, None)),
        out_specs=P(None, "wa", None),
        check_vma=False,
    )
```
